32 devices in a mesh: blk: 8 (over z, y), col: 4 (over x, core).
Axes of the slice: x: 2, y: 2, z: 4, core: 2. Of those that a mesh axis runs over, the one named last changes fastest.
Arguments:
- rank_in: float32 [1024, 512], P(('blk', 'col')), may hold values from 0.5 to 1.5
- delta_in: float32 [1024, 512], P(('blk', 'col'))
- out_degree: int32 [1024, 512], P(('blk', 'col')), may hold values from 26 to 50
- tile_weight: bfloat16 [256, 512, 512], P(('blk', 'col'))
- tile_source: int32 [256], P(('blk', 'col')), may hold values from 0 to 255, as said below
- tile_row: int32 [256], P(('blk', 'col')), may hold values from 0 to 127
- tile_valid: int32 [256], P(('blk', 'col')), may hold values 0 or 1
Outputs:
- rank_out: float32 [1024, 512], P(('blk', 'col'))
- delta_out: float32 [1024, 512], P(('blk', 'col'))
- masses: float32 [6], replicated
The draws below stay inside these ranges and needn't reach their ends.
Inputs may be any that keep to these rules, and one draw needn't show every extreme that they name: `tile_source`: slot j of the 8 slots of each device (tiles i with i % 8 = j) names a source block from 32 * j to 32 * j + 31.
All inputs are finite; a program needn't handle non-finite values. No bound on the sum of `tile_valid` on one device may be relied on, other than what follows from the above.
Results may differ from the reference program's by a relative error of at most 0.00039.
Values may be sent and summed in bfloat16 or wider, within the bound.
A program may use at most 64 MiB of HBM per device.

```python
import jax
import jax.numpy as jnp
from jax import lax

BLOCK = 512
VB = 32
ITERS = 6
NB = 1024
TILES = 256
N_BLK = 8
N_COL = 4


def draw_delta_in(key, part):
    first, second = jax.random.split(jax.random.fold_in(key, 11))
    place = jnp.arange(NB, dtype=jnp.float32) / NB
    rise = 1.0 + 2.0 * place
    rough = jax.random.uniform(second, (NB, 1), jnp.float32, 0.5, 1.5)
    base = jax.random.normal(first, (NB, BLOCK), jnp.float32) + 0.5
    return base * rise[:, None] * rough


def draw_tile_weight(key, part):
    first, second = jax.random.split(jax.random.fold_in(key, 23))
    links = jax.random.bernoulli(first, 0.5, (TILES, BLOCK, BLOCK)).astype(jnp.float32)
    values = jax.random.uniform(second, (TILES, BLOCK, BLOCK), jnp.float32, 0.2, 1.0)
    return (links * values).astype(jnp.bfloat16)


def draw_tile_source(key, part):
    slots = jnp.arange(TILES, dtype=jnp.int32) % N_BLK
    offset = jax.random.randint(jax.random.fold_in(key, 37), (TILES,), 0, VB).astype(jnp.int32)
    return slots * VB + offset


def touch_ends(values, rng, least, high):
    longest = values.shape.index(max(values.shape))
    spots = []
    for shift in (0, 1):
        where = [jax.random.randint(jax.random.fold_in(rng, axis), (), 0, length) for axis, length in enumerate(values.shape)]
        where[longest] = (where[longest] + shift) % values.shape[longest]
        spots.append(tuple(where))
    return values.at[spots[0]].set(least).at[spots[1]].set(high)


def steps_of(rng, shape, cuts, smallest, high):
    gain, own = 1.0, jax.random.fold_in(rng, 6)
    for position, shards_of in cuts:
        heights = jnp.exp(jax.random.uniform(jax.random.fold_in(own, position), (shards_of,), jnp.float32, smallest / len(cuts), high / len(cuts)))
        gain = gain * jnp.repeat(heights, shape[position] // shards_of).reshape([-1 if axis == position else 1 for axis in range(len(shape))])
    return gain


def setup_inputs(seed: int = 0) -> dict:
    seeds = jax.random.split(jax.random.key(seed), 8)
    return {
        "rank_in": jnp.clip(0.5 + 1.0 * jax.random.uniform(seeds[0], (NB, BLOCK), jnp.float32) ** steps_of(seeds[0], (NB, BLOCK), ((0, 32),), -0.2, 0.2), 0.5, 1.5),
        "delta_in": draw_delta_in(jax.random.fold_in(seeds[7], 71), 0),
        "out_degree": touch_ends(jax.random.randint(seeds[2], (NB, BLOCK), 3 * BLOCK * N_BLK // (16 * VB) + 2, 3 * BLOCK * N_BLK // (8 * VB) + 3), jax.random.fold_in(seeds[2], 1), 3 * BLOCK * N_BLK // (16 * VB) + 2, (3 * BLOCK * N_BLK // (8 * VB) + 3) - 1).astype(jnp.int32),
        "tile_weight": draw_tile_weight(jax.random.fold_in(seeds[7], 71), 0),
        "tile_source": draw_tile_source(jax.random.fold_in(seeds[7], 71), 0),
        "tile_row": touch_ends(jax.random.randint(seeds[5], (TILES,), 0, N_COL * VB), jax.random.fold_in(seeds[5], 1), 0, (N_COL * VB) - 1).astype(jnp.int32),
        "tile_valid": touch_ends((jax.random.randint(seeds[6], (TILES,), 0, 4) < 3).astype(jnp.int32), jax.random.fold_in(seeds[6], 1), 0, 1),
    }


damping = 0.85


def reference(rank_in, delta_in, out_degree, tile_weight, tile_source, tile_row, tile_valid):
    slots = jnp.arange(TILES, dtype=jnp.int32)
    device = slots // N_BLK
    group = device // N_COL
    column = device % N_COL
    dest = (group * (N_COL * VB) + tile_row).astype(jnp.int32)
    src = ((tile_source // VB) * (N_COL * VB) + column * VB + tile_source % VB).astype(jnp.int32)
    scale = damping / out_degree.astype(jnp.float32)
    valid = tile_valid.astype(jnp.float32)
    delta = delta_in
    total = rank_in
    masses = []
    for step in range(ITERS):
        masses.append(jnp.sum(jnp.abs(delta)) / (NB * BLOCK))
        total = total + delta
        contrib = (delta * scale).astype(jnp.bfloat16)

        def one_tile(items):
            tile, source = items
            vector = contrib[source].astype(jnp.float32)
            return jnp.dot(tile.astype(jnp.float32), vector, precision=lax.Precision.HIGHEST)

        products = lax.map(one_tile, (tile_weight, src))
        products = products * valid[:, None]
        delta = jnp.zeros((NB, BLOCK), jnp.float32).at[dest].add(products)
    return total, delta, jnp.stack(masses)
```

```python
import functools

import jax
import jax.numpy as jnp
from jax import lax
from jax.experimental import pallas as pl
from jax.experimental.pallas import tpu as pltpu
from jax.sharding import PartitionSpec as P

ITERS = 6
damping = 0.85
MESH = pl.DeviceIdType.MESH
F32 = jnp.float32
BF16 = jnp.bfloat16


def exact_pick(onehot, values):
    high = values.astype(BF16)
    rest = values - high.astype(F32)
    middle = rest.astype(BF16)
    low = (rest - middle.astype(F32)).astype(BF16)
    return (
        jnp.dot(onehot, high, preferred_element_type=F32)
        + jnp.dot(onehot, middle, preferred_element_type=F32)
    ) + jnp.dot(onehot, low, preferred_element_type=F32)


def kernel(
    nb,
    nc,
    rank_hbm,
    delta_hbm,
    degree_hbm,
    weight_hbm,
    source_ref,
    row_ref,
    valid_ref,
    total,
    delta,
    masses_ref,
    weight,
    degree,
    request,
    requests,
    reply,
    replies,
    pick,
    place,
    x_scale,
    rows_out,
    rows_in,
    prods_out,
    prods_in,
    mass_out,
    mass_in,
    load_sem,
    req_sem,
    reply_send,
    reply_recv,
    rows_send,
    rows_recv,
    prods_send,
    prods_recv,
    mass_sem,
):
    nd = nb * nc
    b, c = lax.axis_index("blk"), lax.axis_index("col")
    me = b * nc + c
    slots = weight.shape[0]
    owned, width = delta.shape
    lanes = request.shape[1]
    chunks = width // 128

    loads = [
        pltpu.make_async_copy(src, dst, load_sem.at[i])
        for i, (src, dst) in enumerate(
            ((delta_hbm, delta), (degree_hbm, degree), (rank_hbm, total), (weight_hbm, weight))
        )
    ]
    for load in loads:
        load.start()

    def others(send):
        def step(off, carry):
            dst = lax.rem(me + off, nd)
            send(dst, (lax.div(dst, nc), lax.rem(dst, nc)))
            return carry

        lax.fori_loop(1, nd, step, 0)

    def remote(src, dst, send_sem, recv_sem, device):
        pltpu.make_async_remote_copy(
            src_ref=src,
            dst_ref=dst,
            send_sem=send_sem,
            recv_sem=recv_sem,
            device_id=device,
            device_id_type=MESH,
        ).start()

    def await_bytes(ref, sem):
        pltpu.make_async_copy(ref, ref, sem).wait()

    barrier = pltpu.get_barrier_semaphore()
    others(
        lambda dst, device: pl.semaphore_signal(
            barrier, inc=1, device_id=device, device_id_type=MESH
        )
    )

    lane = lax.broadcasted_iota(jnp.int32, (1, lanes), 1)
    rows = [row_ref[t] * valid_ref[t] + (valid_ref[t] - 1) for t in range(slots)]
    note = jnp.zeros((1, lanes), jnp.int32)
    for t in range(slots):
        note = jnp.where(lane == c * slots + t, rows[t], note)
        note = jnp.where(lane == nc * slots + t, source_ref[t] - t * owned, note)
    request[...] = note.astype(F32)

    pl.semaphore_wait(barrier, nd - 1)

    def ask(off, carry):
        group = lax.rem(b + off, nb)
        remote(request, requests.at[me], req_sem.at[0], req_sem.at[1], (group, c))
        return carry

    lax.fori_loop(1, nb, ask, 0)
    pltpu.make_async_copy(request, requests.at[me], req_sem.at[1]).start()

    def tell(off, carry):
        column = lax.rem(c + lax.rem(off, nc - 1) + 1, nc)
        group = lax.rem(b + lax.div(off, nc - 1), nb)
        remote(request, requests.at[me], req_sem.at[0], req_sem.at[2], (group, column))
        return carry

    lax.fori_loop(0, nb * (nc - 1), tell, 0)

    loads[0].wait()
    loads[1].wait()
    loads[2].wait()
    mass_lane = lax.broadcasted_iota(jnp.int32, (1, 128), 1)

    def account(step, now, masses):
        total[...] = total[...] + now
        mass = jnp.sum(jnp.sum(jnp.abs(now), axis=0, keepdims=True), axis=1, keepdims=True)
        return jnp.where(mass_lane == step, mass, masses)

    masses = account(0, delta[...], jnp.zeros((1, 128), F32))

    def offsets(asked):
        every = lax.broadcasted_iota(jnp.int32, asked.shape, 1)
        return jnp.sum(jnp.where(every == nc * slots + b, asked, 0.0), axis=1, keepdims=True)

    await_bytes(requests.at[pl.ds(0, nb)], req_sem.at[1])
    wanted = offsets(jnp.concatenate([requests[j * nc + c] for j in range(nb)], axis=0))

    owned_lane = lax.broadcasted_iota(jnp.int32, (nb, owned), 1).astype(F32)
    gather = jnp.where(wanted == owned_lane, 1.0, 0.0).astype(BF16)
    first = exact_pick(gather, delta[...])
    under = exact_pick(gather, degree[...].astype(F32))
    for j in range(nb):
        reply[j, :, :width] = first[j : j + 1]
        reply[j, :, width:] = under[j : j + 1]

    def answer(off, carry):
        group = lax.rem(b + off, nb)
        remote(reply.at[group], replies.at[b], reply_send, reply_recv.at[b], (group, c))
        return carry

    lax.fori_loop(1, nb, answer, 0)
    pltpu.make_async_copy(reply.at[b], replies.at[b], reply_recv.at[b]).start()

    await_bytes(requests.at[pl.ds(0, nd - nb)], req_sem.at[2])
    offset = offsets(jnp.concatenate([requests[d] for d in range(nd)], axis=0))

    height = pick.shape[1]
    line = lax.broadcasted_iota(jnp.int32, (height, 128), 0)
    want = jnp.concatenate([offset, jnp.full((height - nd, 1), -2.0 * nd * owned, F32)], axis=0)
    want = jnp.broadcast_to(want, (height, 128)) + (lax.rem(line, nc) * owned).astype(F32)
    for t in range(slots):
        hit = jnp.where(want == rows[t].astype(F32), 1.0, 0.0)
        pick[t] = jnp.where(line < nd, hit, jnp.where(line == nd + t, 1.0, 0.0))

    reach = requests[b * nc]
    for k in range(1, nc):
        reach = reach + requests[b * nc + k]
    mine = lax.broadcasted_iota(jnp.int32, (owned, nc * slots), 0) + c * owned
    place[...] = jnp.where(mine.astype(F32) == reach[:, : nc * slots], 1.0, 0.0).astype(BF16)

    def nearest(k):
        edge = jnp.minimum(b, nb - 1 - b)
        inner = b + (k + 1) // 2 * (1 if k % 2 else -1)
        outer = jnp.where(2 * b < nb, k, nb - 1 - k)
        return jnp.where(2 * edge >= k, inner, outer)

    loads[3].wait()

    def multiply(step, masses, begin, last):
        result = jnp.zeros((height, width), F32)
        for k in range(nb):
            if not begin and k == (0 if last else 0):
                masses = account(step, gather_owned(step - 1), masses)
                if last:
                    spread(masses)
            t = nearest(k)
            if begin:
                await_bytes(replies.at[t], reply_recv.at[t])
                x_scale[t] = damping / replies[t, :, width:]
                x = replies[t, :, :width]
            else:
                if k % 2 == 0:
                    for i in range(k, min(k + 2, nb)):
                        u = nearest(i)
                        group = rows_in.at[step - 1, pl.ds(u * nc, nc)]
                        await_bytes(group, rows_recv.at[step - 1, u])
                x = rows_in[step - 1, t * nc]
                for i in range(1, nc):
                    x = x + rows_in[step - 1, t * nc + i]
            left = jnp.concatenate([pick[t]] * chunks, axis=1) * (x * x_scale[t])
            result = result + lax.dot_general(
                left.astype(BF16),
                weight[t],
                (((1,), (1,)), ((), ())),
                preferred_element_type=F32,
            )
        if not last:
            for d in range(nd):
                rows_out[step, d] = result[d : d + 1]
            for k in reversed(range(nb)):
                g = nearest(k)
                for i in range(1 if k == 0 else 0, nc):
                    e = lax.rem(c + i, nc)
                    remote(
                        rows_out.at[step, g * nc + e],
                        rows_in.at[step, me],
                        rows_send.at[step],
                        rows_recv.at[step, b],
                        (g, e),
                    )
            pltpu.make_async_copy(
                rows_out.at[step, me], rows_in.at[step, me], rows_recv.at[step, b]
            ).start()
        prods_out[step] = result[nd : nd + slots]
        for k in range(1, nc):
            remote(
                prods_out.at[step],
                prods_in.at[step, c],
                prods_send.at[step],
                prods_recv.at[step],
                (b, lax.rem(c + k, nc)),
            )
        pltpu.make_async_copy(
            prods_out.at[step], prods_in.at[step, c], prods_recv.at[step]
        ).start()
        return masses

    def gather_owned(step):
        await_bytes(prods_in.at[step], prods_recv.at[step])
        return exact_pick(place[...], prods_in[step].reshape(nc * slots, width))

    def spread(masses):
        mass_out[...] = masses
        others(
            lambda dst, device: remote(
                mass_out, mass_in.at[me], mass_sem.at[0], mass_sem.at[1], device
            )
        )
        pltpu.make_async_copy(mass_out, mass_in.at[me], mass_sem.at[1]).start()

    masses = multiply(0, masses, True, False)
    masses = lax.fori_loop(
        1, ITERS - 1, lambda step, masses: multiply(step, masses, False, False), masses
    )
    multiply(ITERS - 1, masses, False, True)
    delta[...] = gather_owned(ITERS - 1)

    await_bytes(mass_in, mass_sem.at[1])
    summed = mass_in[0]
    for d in range(1, nd):
        summed = summed + mass_in[d]
    summed = summed / float(nd * owned * width)
    masses_ref[...] = summed

    await_bytes(requests.at[pl.ds(0, nd - 1)], req_sem.at[0])
    await_bytes(replies.at[pl.ds(0, nb - 1)], reply_send)
    await_bytes(mass_in.at[pl.ds(0, nd - 1)], mass_sem.at[0])
    for step in range(ITERS):
        if step < ITERS - 1:
            await_bytes(rows_out.at[step, pl.ds(0, nd - 1)], rows_send.at[step])
        await_bytes(prods_in.at[step, pl.ds(0, nc - 1)], prods_send.at[step])


def finish(total, delta, masses, total_hbm, out_hbm, masses_hbm, mass, sem):
    stores = [
        pltpu.make_async_copy(total, total_hbm, sem.at[0]),
        pltpu.make_async_copy(delta, out_hbm, sem.at[1]),
        pltpu.make_async_copy(mass, masses_hbm, sem.at[2]),
    ]
    stores[0].start()
    stores[1].start()
    lane = lax.broadcasted_iota(jnp.int32, (1, 128), 1)
    for t in range(ITERS):
        mass[t] = jnp.sum(jnp.where(lane == t, masses[...], 0.0))
    stores[2].start()
    for store in stores:
        store.wait()


def on_device(rank_in, delta_in, out_degree, tile_weight, tile_source, tile_row, tile_valid):
    owned, width = delta_in.shape
    slots = tile_weight.shape[0]
    nb = lax.axis_size("blk")
    nc = lax.axis_size("col")
    nd = nb * nc
    lanes = -(-(slots * (nc + 1)) // 128) * 128
    height = -(-(nd + slots) // 16) * 16
    hbm = pl.BlockSpec(memory_space=pl.ANY)
    smem = pl.BlockSpec(memory_space=pltpu.SMEM)
    vmem = pl.BlockSpec(memory_space=pltpu.VMEM)
    dma = pltpu.SemaphoreType.DMA
    total, delta, masses = pl.pallas_call(
        functools.partial(kernel, nb, nc),
        out_shape=(
            pltpu.VMEM((owned, width), F32),
            pltpu.VMEM((owned, width), F32),
            pltpu.VMEM((1, 128), F32),
        ),
        in_specs=[hbm] * 4 + [smem] * 3,
        out_specs=(vmem, vmem, vmem),
        scratch_shapes=[
            pltpu.VMEM((slots, width, width), BF16),
            pltpu.VMEM((owned, width), jnp.int32),
            pltpu.VMEM((1, lanes), F32),
            pltpu.VMEM((nd, 1, lanes), F32),
            pltpu.VMEM((nb, 1, 2 * width), F32),
            pltpu.VMEM((nb, 1, 2 * width), F32),
            pltpu.VMEM((slots, height, 128), F32),
            pltpu.VMEM((owned, nc * slots), BF16),
            pltpu.VMEM((nb, 1, width), F32),
            pltpu.VMEM((ITERS - 1, nd, 1, width), F32),
            pltpu.VMEM((ITERS - 1, nd, 1, width), F32),
            pltpu.VMEM((ITERS, slots, width), F32),
            pltpu.VMEM((ITERS, nc, slots, width), F32),
            pltpu.VMEM((1, 128), F32),
            pltpu.VMEM((nd, 1, 128), F32),
            dma((4,)),
            dma((3,)),
            dma,
            dma((nb,)),
            dma((ITERS - 1,)),
            dma((ITERS - 1, nb)),
            dma((ITERS,)),
            dma((ITERS,)),
            dma((2,)),
        ],
        compiler_params=pltpu.CompilerParams(
            collective_id=0, has_side_effects=True, vmem_limit_bytes=60 * 1024 * 1024
        ),
    )(rank_in, delta_in, out_degree, tile_weight, tile_source, tile_row, tile_valid)
    return pl.pallas_call(
        finish,
        out_shape=(
            jax.ShapeDtypeStruct((owned, width), F32),
            jax.ShapeDtypeStruct((owned, width), F32),
            jax.ShapeDtypeStruct((ITERS,), F32),
        ),
        in_specs=[vmem] * 3,
        out_specs=(hbm, hbm, hbm),
        scratch_shapes=[pltpu.SMEM((ITERS,), F32), dma((3,))],
        compiler_params=pltpu.CompilerParams(vmem_limit_bytes=4 * 1024 * 1024),
    )(total, delta, masses)


def solution(mesh):
    return jax.shard_map(
        on_device,
        mesh=mesh,
        in_specs=(
            P(("blk", "col"), None),
            P(("blk", "col"), None),
            P(("blk", "col"), None),
            P(("blk", "col"), None, None),
            P(("blk", "col")),
            P(("blk", "col")),
            P(("blk", "col")),
        ),
        out_specs=(P(("blk", "col"), None), P(("blk", "col"), None), P()),
        check_vma=False,
    )
```
